32 devices in a mesh: groups: 2 (over x), ctx: 16 (over z, y, core).
Axes of the slice: x: 2, y: 2, z: 4, core: 2. Of those that a mesh axis runs over, the one named last changes fastest.
Arguments:
- queries: bfloat16 [8192, 1024], P(('groups', 'ctx')), parts along dimension 0, may hold values from -7 to 7
- keys: bfloat16 [8192, 128], P(('groups', 'ctx')), parts along dimension 0, may hold values from -7 to 7
- values: bfloat16 [8192, 128], P(('groups', 'ctx')), parts along dimension 0, may hold values from -6 to 6
- span_order: int32 [64], P('groups'), parts along dimension 0, may hold values from 0 to 31, as said below
Outputs:
- attended: bfloat16 [8192, 1024], P(('groups', 'ctx')), parts along dimension 0
The draws below stay inside these ranges and needn't reach their ends.
There are 2 independent parts, one for each index of `groups`. The reference program is written for one: setup_inputs(seed, part) draws one part's arguments, and reference() takes and returns one part's arrays. A program takes and returns all parts, laid end to end along the dimension named above; each array names one. Nothing has to cross between parts.
Inputs may be any that keep to these rules, and one draw needn't show every extreme that they name: A permutation: rows j * 128 to (j + 1) * 128 - 1 hold span span_order[j] of the sequence; for every j, span_order[2 j] + span_order[2 j + 1] = 31.
All inputs are finite; a program needn't handle non-finite values.
Results may differ from the reference program's by a relative error of at most 0.006.
Values may be sent and summed in bfloat16 or wider, within the bound.
No kernel may reach another device: no remote copies, remote signals or barrier semaphores. Data moves between devices by JAX's collectives and lax.ppermute only.
A program may use at most 64 MiB of HBM per device.

```python
import math
import jax
import jax.numpy as jnp
from jax import lax

QH = 8
DH = 128
SPAN = 128
SEQ = 4096
NSPAN = 32


def drawn_pair(key):
    query_key = jax.random.fold_in(key, 11)
    keys_key = jax.random.fold_in(key, 12)
    query_draw = jnp.clip(jax.random.normal(query_key, (SEQ, QH * DH), jnp.float32), -5.0, 5.0)
    keys_draw = jnp.clip(jax.random.normal(keys_key, (SEQ, DH), jnp.float32), -5.0, 5.0)
    return (query_draw, keys_draw)


def draw_queries(key, part):
    return drawn_pair(key)[0].astype(jnp.bfloat16)


def draw_keys(key, part):
    return drawn_pair(key)[1].astype(jnp.bfloat16)


def draw_span_order(key, part):
    half = NSPAN // 2
    pairs = jax.random.permutation(jax.random.fold_in(key, 21), half).astype(jnp.int32)
    flipped = jax.random.randint(jax.random.fold_in(key, 22), (half,), 0, 2)
    early = pairs
    late = (NSPAN - 1 - pairs).astype(jnp.int32)
    first = jnp.where(flipped == 1, late, early)
    second = jnp.where(flipped == 1, early, late)
    return jnp.stack([first, second], axis=1).reshape(NSPAN).astype(jnp.int32)


def shard_levels(stream_key, shape, cuts, smallest, top_value):
    factor_of = 1.0
    for dim, parts in cuts:
        draws = jax.random.uniform(jax.random.fold_in(jax.random.fold_in(stream_key, 6), dim), (parts,), jnp.float32, smallest / len(cuts), top_value / len(cuts))
        factor_of = factor_of * jnp.repeat(jnp.exp(draws), shape[dim] // parts).reshape((-1,) + (1,) * (len(shape) - 1 - dim))
    return factor_of


def noise(stream_key, shape, width, most, cuts=(), held_as=jnp.bfloat16):
    array = width * jax.random.normal(stream_key, shape, jnp.float32)
    if cuts:
        array = array * shard_levels(stream_key, shape, cuts, -0.22, 0.18)
    return jnp.clip(array, -most, most).astype(held_as)


def setup_inputs(seed: int = 0, part: int = 0) -> dict:
    arg_keys = jax.random.split(jax.random.key(seed), 5)
    own_keys = jax.random.split(jax.random.fold_in(arg_keys[4], part), 5)
    return {
        "queries": draw_queries(jax.random.fold_in(jax.random.fold_in(arg_keys[4], part), 71), part),
        "keys": draw_keys(jax.random.fold_in(jax.random.fold_in(arg_keys[4], part), 71), part),
        "values": noise(own_keys[2], (SEQ, DH), 1.0, 6.0, ((0, 16),)),
        "span_order": draw_span_order(jax.random.fold_in(jax.random.fold_in(arg_keys[4], part), 71), part),
    }


def reference(queries, keys, values, span_order):
    total_rows = queries.shape[0]
    rows = jnp.arange(total_rows, dtype=jnp.int32)
    position = (span_order[rows // SPAN] * SPAN + rows % SPAN).astype(jnp.int32)
    block = math.gcd(total_rows, 512)
    scale = 1.0 / math.sqrt(DH)
    keys_f = keys.astype(jnp.float32)
    values_f = values.astype(jnp.float32)

    def one_block(index):
        first = (index * block).astype(jnp.int32)
        query_blk = lax.dynamic_slice_in_dim(queries, first, block, 0).reshape(block, QH, DH).astype(jnp.float32)
        query_pos = lax.dynamic_slice_in_dim(position, first, block, 0)
        score = jnp.einsum('qhd,kd->hqk', query_blk, keys_f) * scale
        kept = position[None, None, :] <= query_pos[None, :, None]
        score = jnp.where(kept, score, jnp.float32(-1e+30))
        top = lax.optimization_barrier(jnp.max(score, axis=-1, keepdims=True))
        weight = jnp.where(kept, jnp.exp(score - top), jnp.float32(0.0))
        total = lax.optimization_barrier(jnp.sum(weight, axis=-1))
        weight_b = lax.optimization_barrier(weight.astype(jnp.bfloat16)).astype(jnp.float32)
        mixed = jnp.einsum('hqk,kd->hqd', weight_b, values_f) / total[:, :, None]
        return jnp.transpose(mixed, (1, 0, 2)).reshape(block, QH * DH).astype(jnp.bfloat16)
    outputs = lax.map(one_block, jnp.arange(total_rows // block, dtype=jnp.int32))
    return outputs.reshape(total_rows, QH * DH)
```

```python
import functools
import math

import jax
import jax.numpy as jnp
from jax import lax
from jax.experimental import pallas as pl
from jax.experimental.pallas import tpu as pltpu
from jax.sharding import PartitionSpec as P


F32 = jnp.float32
BF16 = jnp.bfloat16
VMEM = pl.BlockSpec(memory_space=pltpu.VMEM)
SMEM = pl.BlockSpec(memory_space=pltpu.SMEM)
AUG = 16
LIMIT = 2.0**100
LATE, EARLY = 0, 1


def spans_of(order, device):
    first, second = order[2 * device], order[2 * device + 1]
    return jnp.minimum(first, second), jnp.maximum(first, second), first < second


def offsets(first_is_early, span):
    early = pl.multiple_of(jnp.where(first_is_early, 0, span), span)
    late = pl.multiple_of(jnp.where(first_is_early, span, 0), span)
    return early, late


def product(keys, qh, ql):
    return jnp.dot(
        jnp.concatenate([keys, keys], 1),
        jnp.concatenate([qh, ql], 0),
        preferred_element_type=F32,
    )


def weighted(values_t, weight):
    ones = jnp.ones((AUG, values_t.shape[1]), BF16)
    return jnp.dot(
        jnp.concatenate([values_t, ones], 0), weight.astype(BF16), preferred_element_type=F32
    )


def pack_kernel(k_ref, v_ref, out_ref):
    rows, span = k_ref.shape[0], k_ref.shape[0] // 2
    out_ref[0:rows, :] = k_ref[...]
    for i in range(2):
        at = i * span
        out_ref[rows + at : rows + at + span, :] = v_ref[at : at + span, :].T


def own_kernel(heads, order, q_ref, kv_ref, qh_ref, ql_ref, m_ref, acc_ref):
    rows = q_ref.shape[0]
    span = rows // 2
    size = kv_ref.shape[1]
    me = lax.axis_index("ctx")
    _, _, first_is_early = spans_of(order, me)
    early, late = offsets(first_is_early, span)
    scale = math.log2(math.e) / math.sqrt(size)
    for half, at in ((LATE, late), (EARLY, early)):
        for h in range(heads):
            q = q_ref[pl.ds(at, span), h * size : (h + 1) * size].astype(F32).T * scale
            hi = q.astype(BF16)
            qh_ref[half, :, h * span : (h + 1) * span] = hi
            ql_ref[half, :, h * span : (h + 1) * span] = (q - hi.astype(F32)).astype(BF16)
    k_early, k_late = kv_ref[pl.ds(early, span), :], kv_ref[pl.ds(late, span), :]
    v_early = kv_ref[pl.ds(rows + early, span), :]
    v_late = kv_ref[pl.ds(rows + late, span), :]
    cols = heads * span
    key = lax.broadcasted_iota(jnp.int32, (span, cols), 0)
    query = lax.broadcasted_iota(jnp.int32, (span, cols), 1) % span
    kept = key <= query
    diagonal = jnp.where(kept, product(k_late, qh_ref[LATE], ql_ref[LATE]), -1e30)
    full = product(k_early, qh_ref[LATE], ql_ref[LATE])
    m = jnp.max(jnp.maximum(diagonal, full), axis=0, keepdims=True)
    m_ref[LATE] = jnp.broadcast_to(m, m_ref.shape[1:])
    weight = jnp.concatenate(
        [jnp.exp2(full - m), jnp.where(kept, jnp.exp2(diagonal - m), 0.0)], 0
    )
    acc_ref[LATE] = weighted(jnp.concatenate([v_early, v_late], 1), weight)
    diagonal = jnp.where(kept, product(k_early, qh_ref[EARLY], ql_ref[EARLY]), -1e30)
    m = jnp.max(diagonal, axis=0, keepdims=True)
    m_ref[EARLY] = jnp.broadcast_to(m, m_ref.shape[1:])
    acc_ref[EARLY] = weighted(v_early, jnp.where(kept, jnp.exp2(diagonal - m), 0.0))


def attend(keys, values_t, half, qh_ref, ql_ref, m_ref, acc_ref):
    score = product(keys, qh_ref[half], ql_ref[half])
    acc_ref[half] += weighted(values_t, jnp.exp2(score - m_ref[half, 0:1, :]))


def group(order, masks, blocks, qh_ref, ql_ref, m_ref, acc_ref):
    rows = blocks[0].shape[0] // 2
    span = rows // 2
    me = lax.axis_index("ctx")
    mine, _, _ = spans_of(order, me)
    for i in range(0, len(blocks), 2):
        keys, values = [], []
        later = []
        for mask, block in zip(masks[i : i + 2], blocks[i : i + 2]):
            theirs, _, first_is_early = spans_of(order, me ^ mask)
            early, late = offsets(first_is_early, span)
            keys.append(block[pl.ds(early, span), :])
            values.append(block[pl.ds(rows + early, span), :])
            below = theirs < mine
            at = pl.multiple_of(jnp.where(below, early, late), span)
            later.append((block, at, jnp.where(below, EARLY, LATE)))
        attend(
            jnp.concatenate(keys, 0), jnp.concatenate(values, 1), LATE,
            qh_ref, ql_ref, m_ref, acc_ref,
        )
        for block, at, half in later:
            attend(
                block[pl.ds(at, span), :], block[pl.ds(rows + at, span), :], half,
                qh_ref, ql_ref, m_ref, acc_ref,
            )


def careful(order, masks, blocks, qh_ref, ql_ref, acc_ref, held, top):
    rows = blocks[0].shape[0] // 2
    span = rows // 2
    cols = qh_ref.shape[2]
    me = lax.axis_index("ctx")
    mine_early, mine_late, _ = spans_of(order, me)
    top[...] = jnp.full_like(top, -1e30)
    acc_ref[...] = jnp.zeros_like(acc_ref)
    for mask, block in zip(masks, blocks):
        held[...] = block[...]
        device = me ^ mask

        def step(i, _):
            at = pl.multiple_of((i // 2) * span, span)
            half = i % 2
            key_span = order[2 * device + i // 2]
            query_span = jnp.where(half == LATE, mine_late, mine_early)
            key = key_span * span + lax.broadcasted_iota(jnp.int32, (span, cols), 0)
            row = lax.broadcasted_iota(jnp.int32, (span, cols), 1) % span
            kept = key <= query_span * span + row
            score = product(held[pl.ds(at, span), :], qh_ref[half], ql_ref[half])
            score = jnp.where(kept, score, -1e30)
            before = top[half, 0:1, :]
            after = jnp.maximum(before, jnp.max(score, axis=0, keepdims=True))
            weight = jnp.where(kept, jnp.exp2(score - after), 0.0)
            fresh = weighted(held[pl.ds(rows + at, span), :], weight)
            acc_ref[half] = acc_ref[half] * jnp.exp2(before - after) + fresh
            top[half] = jnp.broadcast_to(after, top.shape[1:])
            return 0

        lax.fori_loop(0, 4, step, 0)


def last_kernel(heads, masks, order, own_ref, *refs):
    count = len(masks)
    blocks = refs[:count]
    qh_ref, ql_ref, m_ref, acc_in, out_ref, acc_ref, held, top = refs[count:]
    size = own_ref.shape[1]
    span = own_ref.shape[0] // 4
    me = lax.axis_index("ctx")
    acc_ref[...] = acc_in[...]
    group(order, masks, blocks, qh_ref, ql_ref, m_ref, acc_ref)
    bad = jnp.max(jnp.where(acc_ref[:, size : size + 8, :] < LIMIT, 0.0, 1.0)) > 0.5

    @pl.when(bad)
    def _():
        careful(order, (0,) + masks, (own_ref,) + blocks, qh_ref, ql_ref, acc_ref, held, top)

    _, _, first_is_early = spans_of(order, me)
    early, late = offsets(first_is_early, span)
    for half, at in ((LATE, late), (EARLY, early)):
        for h in range(heads):
            cols = slice(h * span, (h + 1) * span)
            mixed = acc_ref[half, 0:size, cols] / acc_ref[half, size : size + 1, cols]
            out_ref[pl.ds(at, span), h * size : (h + 1) * size] = mixed.T.astype(BF16)


def body(queries, keys, values, span_order):
    rows = queries.shape[0]
    span = rows // 2
    size = keys.shape[1]
    heads = queries.shape[1] // size
    cols = heads * span
    n = span_order.shape[0] // 2

    def swap(mask, block):
        return lax.ppermute(block, "ctx", [(i, i ^ mask) for i in range(n)])

    half_shape = jax.ShapeDtypeStruct((2, size, cols), BF16)
    top_shape = jax.ShapeDtypeStruct((2, 8, cols), F32)
    acc_shape = jax.ShapeDtypeStruct((2, size + AUG, cols), F32)
    params = pltpu.CompilerParams(vmem_limit_bytes=28 * 2**20)

    own = pl.pallas_call(
        pack_kernel,
        out_shape=jax.ShapeDtypeStruct((2 * rows, size), BF16),
        in_specs=[VMEM, VMEM],
        out_specs=VMEM,
        compiler_params=params,
    )(keys, values)

    column = {}
    for mask in reversed(range(4, n, 4)):
        column[mask] = swap(mask, own)
    column[2] = swap(2, own)
    for mask in reversed(range(4, n, 4)):
        column[mask ^ 2] = swap(2, column[mask])
    blocks = {1: swap(1, own)}
    for mask, block in column.items():
        blocks[mask] = block
        blocks[mask ^ 1] = swap(1, block)

    state = pl.pallas_call(
        functools.partial(own_kernel, heads),
        out_shape=(half_shape, half_shape, top_shape, acc_shape),
        in_specs=[SMEM, VMEM, VMEM],
        out_specs=(VMEM,) * 4,
        compiler_params=params,
    )(span_order, queries, own)
    masks = tuple(blocks)
    return pl.pallas_call(
        functools.partial(last_kernel, heads, masks),
        out_shape=jax.ShapeDtypeStruct(queries.shape, BF16),
        in_specs=[SMEM] + [VMEM] * (len(masks) + 5),
        out_specs=VMEM,
        scratch_shapes=[
            pltpu.VMEM(acc_shape.shape, F32),
            pltpu.VMEM((2 * rows, size), BF16),
            pltpu.VMEM(top_shape.shape, F32),
        ],
        compiler_params=params,
    )(span_order, own, *blocks.values(), *state)


def solution(mesh):
    in_specs = (
        P(("groups", "ctx"), None),
        P(("groups", "ctx"), None),
        P(("groups", "ctx"), None),
        P("groups"),
    )
    out_specs = P(("groups", "ctx"), None)
    return jax.shard_map(body, mesh=mesh, in_specs=in_specs, out_specs=out_specs, check_vma=False)
```
